32 devices in a mesh: slab: 8 (over y, x, core), cross: 4 (over z).
Axes of the slice: x: 2, y: 2, z: 4, core: 2. Of those that a mesh axis runs over, the one named last changes fastest.
Arguments:
- velocity: float32 [3, 32, 64, 128], P(None, 'slab', 'cross'), may hold values from -6 to 6
- density: float32 [32, 64, 128], P('slab', 'cross'), may hold values from 0.5 to 2
- source: float32 [32, 64, 128], P('slab', 'cross'), may hold values from -6 to 6
- species: float32 [9, 32, 64, 128], P(None, 'slab', 'cross'), may hold values from 0 to 1
Outputs:
- velocity_out: float32 [3, 32, 64, 128], P(None, 'slab', 'cross')
- pressure: float32 [32, 64, 128], P('slab', 'cross')
- species_out: float32 [9, 32, 64, 128], P(None, 'slab', 'cross')
The draws below stay inside these ranges and needn't reach their ends.
All inputs are finite; a program needn't handle non-finite values.
Results may differ from the reference program's by a relative error of at most 0.0001.
Values sent between devices are 32-bit elements; how exact they have to be, the bound alone decides.
A program may use at most 64 MiB of HBM per device.

```python
import math
import jax
import jax.numpy as jnp

NZ = 128
SPECIES = 9
CYCLES = 2
SMOOTH = 2
COARSE = 4
NX = 32
NY = 64


def shard_levels(key, shape, pieces, low, largest):
    gain = 1.0
    for axis_at, blocks in pieces:
        heights = jax.random.uniform(jax.random.fold_in(jax.random.fold_in(key, 6), axis_at), (blocks,), jnp.float32, low / len(pieces), largest / len(pieces))
        gain = gain * jnp.repeat(jnp.exp(heights), shape[axis_at] // blocks).reshape((-1,) + (1,) * (len(shape) - 1 - axis_at))
    return gain


def centred(rng, shape, scale, reach, pieces=(), dtype=jnp.bfloat16):
    drawn = jax.random.normal(rng, shape, jnp.float32) * scale
    if len(pieces) > 0:
        drawn = shard_levels(rng, shape, pieces, -0.22, 0.18) * drawn
    return jnp.clip(drawn, min=-reach, max=reach).astype(dtype)


def setup_inputs(seed: int = 0) -> dict:
    key_of = jax.random.split(jax.random.key(seed), 5)
    velocity = centred(key_of[0], (3, NX, NY, NZ), 1.0, 6.0, ((1, 8), (2, 4)), jnp.float32)
    density = jnp.clip(jnp.exp(math.log(2.0) - 1.3862944 * jax.random.uniform(key_of[1], (NX, NY, NZ), jnp.float32) ** shard_levels(key_of[1], (NX, NY, NZ), ((0, 8), (1, 4)), -0.2, 0.2)), 0.5, 2.0)
    source = centred(key_of[2], (NX, NY, NZ), 1.0, 6.0, ((0, 8), (1, 4)), jnp.float32)
    species = jnp.clip(1.0 * jax.random.uniform(key_of[3], (SPECIES, NX, NY, NZ), jnp.float32) ** shard_levels(key_of[3], (SPECIES, NX, NY, NZ), ((1, 8), (2, 4)), -0.2, 0.2), 0.0, 1.0)
    return dict(velocity=velocity, density=density, source=source, species=species)


damping = 0.8
time_step = 0.25


def pad_plane(field, width):
    return jnp.pad(field, ((width, width), (width, width), (0, 0)))


def pad_stack(field, width):
    return jnp.pad(field, ((0, 0), (width, width), (width, width), (0, 0)))


def pad_depth(field):
    return jnp.pad(field, ((0, 0), (0, 0), (1, 1)))


def face_weights(mobile):
    face_x = 0.5 * (mobile[:-1, 1:-1] + mobile[1:, 1:-1])
    face_y = 0.5 * (mobile[1:-1, :-1] + mobile[1:-1, 1:])
    inner = pad_depth(mobile[1:-1, 1:-1])
    face_z = 0.5 * (inner[..., :-1] + inner[..., 1:])
    diagonal = face_x[:-1] + face_x[1:] + face_y[:, :-1] + face_y[:, 1:] + face_z[..., :-1] + face_z[..., 1:]
    return face_x, face_y, face_z, diagonal


def operate(field, weights):
    face_x, face_y, face_z = weights[0], weights[1], weights[2]
    center = field[1:-1, 1:-1]
    column = pad_depth(center)
    total = face_x[1:] * (field[2:, 1:-1] - center) + face_x[:-1] * (field[:-2, 1:-1] - center)
    total = total + face_y[:, 1:] * (field[1:-1, 2:] - center) + face_y[:, :-1] * (field[1:-1, :-2] - center)
    total = total + face_z[..., 1:] * (column[..., 2:] - center) + face_z[..., :-1] * (column[..., :-2] - center)
    return total


def jacobi_step(field, target, weights):
    center = field[1:-1, 1:-1]
    return center + damping * (operate(field, weights) - target) / weights[3]


def divergence(moving):
    column = pad_depth(moving[2][1:-1, 1:-1])
    total = (moving[0][2:, 1:-1] - moving[0][:-2, 1:-1]) + (moving[1][1:-1, 2:] - moving[1][1:-1, :-2])
    return 0.5 * (total + (column[..., 2:] - column[..., :-2]))


def gradient(field):
    column = pad_depth(field[1:-1, 1:-1])
    along_x = 0.5 * (field[2:, 1:-1] - field[:-2, 1:-1])
    along_y = 0.5 * (field[1:-1, 2:] - field[1:-1, :-2])
    along_z = 0.5 * (column[..., 2:] - column[..., :-2])
    return jnp.stack([along_x, along_y, along_z], 0)


def restrict(field):
    cells_x, cells_y, cells_z = field.shape
    return field.reshape(cells_x // 2, 2, cells_y // 2, 2, cells_z // 2, 2).mean(axis=(1, 3, 5))


def prolong(field):
    cells_x, cells_y, cells_z = field.shape
    spread = jnp.broadcast_to(field[:, None, :, None, :, None], (cells_x, 2, cells_y, 2, cells_z, 2))
    return spread.reshape(2 * cells_x, 2 * cells_y, 2 * cells_z)


def advect(amounts, moving):
    flow_x = 0.5 * (moving[0][:-1, 1:-1] + moving[0][1:, 1:-1])
    flux_x = jnp.maximum(flow_x, 0.0) * amounts[:, :-1, 1:-1] + jnp.minimum(flow_x, 0.0) * amounts[:, 1:, 1:-1]
    flow_y = 0.5 * (moving[1][1:-1, :-1] + moving[1][1:-1, 1:])
    flux_y = jnp.maximum(flow_y, 0.0) * amounts[:, 1:-1, :-1] + jnp.minimum(flow_y, 0.0) * amounts[:, 1:-1, 1:]
    column = pad_depth(moving[2][1:-1, 1:-1])
    flow_z = 0.5 * (column[..., :-1] + column[..., 1:])
    center = amounts[:, 1:-1, 1:-1]
    stacked = jnp.pad(center, ((0, 0), (0, 0), (0, 0), (1, 1)))
    flux_z = jnp.maximum(flow_z, 0.0) * stacked[..., :-1] + jnp.minimum(flow_z, 0.0) * stacked[..., 1:]
    change = (flux_x[:, 1:] - flux_x[:, :-1]) + (flux_y[:, :, 1:] - flux_y[:, :, :-1]) + (flux_z[..., 1:] - flux_z[..., :-1])
    return center - time_step * change


def reference(velocity, density, source, species):
    mobility = 1.0 / density
    weights = face_weights(pad_plane(mobility, 1))
    target = divergence(pad_stack(velocity, 1)) - source
    coarse_weights = tuple(0.25 * part for part in face_weights(pad_plane(restrict(mobility), 1)))
    pressure = jnp.zeros_like(density)
    for cycle_index in range(CYCLES):
        for sweep_index in range(SMOOTH):
            pressure = jacobi_step(pad_plane(pressure, 1), target, weights)
        residual = target - operate(pad_plane(pressure, 1), weights)
        coarse_target = restrict(residual)
        correction = jnp.zeros_like(coarse_target)
        for sweep_index in range(COARSE):
            correction = jacobi_step(pad_plane(correction, 1), coarse_target, coarse_weights)
        pressure = pressure + prolong(correction)
        for sweep_index in range(SMOOTH):
            pressure = jacobi_step(pad_plane(pressure, 1), target, weights)
    velocity_out = velocity - mobility[None] * gradient(pad_plane(pressure, 1))
    species_out = advect(pad_stack(species, 1), pad_stack(velocity_out, 1))
    return velocity_out, pressure, species_out
```

```python
import functools

import jax
import jax.numpy as jnp
from jax import lax
from jax.experimental import pallas as pl
from jax.experimental.pallas import tpu as pltpu
from jax.sharding import PartitionSpec as P

CYCLES = 2
COARSE = 4
damping = 0.8
time_step = 0.25
MESH = pl.DeviceIdType.MESH
HX = 4
HY = 8
KY = 4

NEAR = [(dx, dy) for dx in (-1, 0, 1) for dy in (-1, 0, 1) if (dx, dy) != (0, 0)]
WIDE = [(dx, dy) for dx in (-2, -1, 0, 1, 2) for dy in (-1, 0, 1) if (dx, dy) != (0, 0)]
SIDE = [(-1, 0), (1, 0), (0, -1), (0, 1)]


def kernel(
    slabs, crosses, velocity, density, source, species, vel_out, pres_out, spec_out,
    fields, coarse_m, rhs, press, rim_x, rim_y, last,
    xa, xb, ya, yb, za, zb, goal, scale_back, pa, pb,
    cxa, cxb, cya, cyb, cza, czb, cinv, ca, cb,
    f_send, f_recv, m_send, m_recv, r_send, r_recv, p_send, p_recv, s_send, s_recv, l_send, l_recv,
):
    cells_x, cells_y, cells_z = density.shape
    wx, wy = cells_x + 2 * HX, cells_y + 2 * HY
    half = cells_x // 2
    cw = cells_x // 2 + 4 * half
    own_y = pl.ds(HY, cells_y)
    own_x = pl.ds(HX, cells_x)
    own_c = pl.ds(2 * half, half)
    slab, cross = lax.axis_index("slab"), lax.axis_index("cross")
    f32 = jnp.float32

    def there(dx, dy):
        return (slab + dx >= 0) & (slab + dx < slabs) & (cross + dy >= 0) & (cross + dy < crosses)

    def ys(dy, k):
        if dy == 0:
            return own_y, own_y
        if dy > 0:
            return pl.ds(HY + cells_y - k, k), pl.ds(HY - k, k)
        return pl.ds(HY, k), pl.ds(HY + cells_y, k)

    def fine_cut(ref, dx, dy, k, lead):
        sy, dyy = ys(dy, k)
        dst_x = pl.ds(HX - dx * cells_x, cells_x)
        pre = (slice(None),) if lead else ()
        return ref.at[pre + (own_x, sy)], ref.at[pre + (dst_x, dyy)]

    def coarse_cut(ref, dx, dy, at=None):
        sy, dyy = ys(dy, HY)
        dst_x = pl.ds(2 * half - dx * half, half)
        pre = () if at is None else (at,)
        return ref.at[pre + (own_c, sy)], ref.at[pre + (dst_x, dyy)]

    def exchange(directions, cut, send, recv):
        def copy(index, dx, dy):
            src, dst = cut(dx, dy)
            return pltpu.make_async_remote_copy(
                src_ref=src, dst_ref=dst, send_sem=send.at[index], recv_sem=recv.at[index],
                device_id=(slab + dx, cross + dy), device_id_type=MESH,
            )

        def start():
            for index, (dx, dy) in enumerate(directions):
                @pl.when(there(dx, dy))
                def _():
                    copy(index, dx, dy).start()

        def arrive():
            for index, (dx, dy) in enumerate(directions):
                @pl.when(there(-dx, -dy))
                def _():
                    copy(index, dx, dy).wait_recv()

        def leave():
            for index, (dx, dy) in enumerate(directions):
                @pl.when(there(dx, dy))
                def _():
                    copy(index, dx, dy).wait_send()

        return start, arrive, leave

    f_x = exchange(NEAR, lambda dx, dy: fine_cut(fields, dx, dy, KY, True), f_send, f_recv)
    m_x = exchange(WIDE, lambda dx, dy: coarse_cut(coarse_m, dx, dy), m_send, m_recv)
    r_x = [
        exchange(WIDE, lambda dx, dy, at=at: coarse_cut(rhs, dx, dy, at), r_send.at[at], r_recv.at[at])
        for at in range(CYCLES)
    ]
    p_x = exchange(NEAR, lambda dx, dy: fine_cut(press, dx, dy, KY, False), p_send, p_recv)

    def last_cut(dx, dy):
        if dx != 0:
            src = pl.ds(HX + cells_x - 2, 2) if dx > 0 else pl.ds(HX, 2)
            dst = pl.ds(HX - 2, 2) if dx > 0 else pl.ds(HX + cells_x, 2)
            return last.at[src, own_y], last.at[dst, own_y]
        sy, dyy = ys(dy, 2)
        return last.at[own_x, sy], last.at[own_x, dyy]

    l_x = exchange(SIDE, last_cut, l_send, l_recv)

    def species_cut(dx, dy):
        if dx != 0:
            return species.at[:, cells_x - 1 if dx > 0 else 0], rim_x.at[0 if dx > 0 else 1]
        row = cells_y - 1 if dy > 0 else 0
        return species.at[:, :, pl.ds(row, 1)], rim_y.at[0 if dy > 0 else 1, :, :, pl.ds(0, 1)]

    s_x = exchange(SIDE, species_cut, s_send, s_recv)

    def grids(rows):
        lane = lax.broadcasted_iota(jnp.int32, (rows, cells_z), 1)
        row = lax.broadcasted_iota(jnp.int32, (rows, cells_z), 0)
        return row, lane

    def next_z(v, k=1):
        return pltpu.roll(v, cells_z - k, 1)

    def prev_z(v, k=1):
        return pltpu.roll(v, k, 1)

    def next_y(v, k=1):
        return pltpu.roll(v, v.shape[0] - k, 0)

    def prev_y(v, k=1):
        return pltpu.roll(v, k, 0)

    row_w, lane_w = grids(wy)
    row_o, lane_o = grids(cells_y)

    def pair_sum(v, row, lane):
        v = v + jnp.where(row % 2 == 0, next_y(v), prev_y(v))
        return v + jnp.where(lane % 2 == 0, next_z(v), prev_z(v))

    for ref in (fields, coarse_m, rhs, press, rim_x, rim_y, last):
        ref[...] = jnp.zeros(ref.shape, f32)
    for x in range(cells_x):
        v2 = velocity[2, x]
        dz = jnp.where(lane_o == cells_z - 1, 0.0, next_z(v2)) - jnp.where(lane_o == 0, 0.0, prev_z(v2))
        fields[0, HX + x, own_y] = 1.0 / density[x]
        fields[1, HX + x, own_y] = velocity[0, x]
        fields[2, HX + x, own_y] = velocity[1, x]
        fields[3, HX + x, own_y] = 0.5 * dz - source[x]
    for c in range(half):
        m = 1.0 / density[2 * c] + 1.0 / density[2 * c + 1]
        coarse_m[2 * half + c, own_y] = 0.125 * pair_sum(m, row_o, lane_o)

    barrier = pltpu.get_barrier_semaphore()
    count = jnp.int32(0)
    for dx, dy in WIDE:
        here = there(dx, dy)
        count = count + here.astype(jnp.int32)

        @pl.when(here)
        def _():
            pl.semaphore_signal(barrier, inc=1, device_id=(slab + dx, cross + dy), device_id_type=MESH)

    pl.semaphore_wait(barrier, count)
    f_x[0]()
    m_x[0]()
    s_x[0]()
    f_x[1]()

    for x in range(1, wx - 1):
        m = fields[0, x]
        lo_x, hi_x = 0.5 * (m + fields[0, x - 1]), 0.5 * (m + fields[0, x + 1])
        lo_y, hi_y = 0.5 * (m + prev_y(m)), 0.5 * (m + next_y(m))
        lo_z = 0.5 * (m + jnp.where(lane_w == 0, 0.0, prev_z(m)))
        hi_z = 0.5 * (m + jnp.where(lane_w == cells_z - 1, 0.0, next_z(m)))
        diag = lo_x + hi_x + lo_y + hi_y + lo_z + hi_z
        inside = m > 0.0
        inv = jnp.where(inside, damping / jnp.where(inside, diag, 1.0), 0.0)
        xa[x], xb[x] = lo_x * inv, hi_x * inv
        ya[x], yb[x] = lo_y * inv, hi_y * inv
        za[x] = jnp.where(lane_w == 0, 0.0, lo_z * inv)
        zb[x] = jnp.where(lane_w == cells_z - 1, 0.0, hi_z * inv)
        if HX <= x < HX + cells_x:
            scale_back[x - HX] = (diag * (1.0 / damping))[HY : HY + cells_y]
        v1 = fields[2, x]
        t = 0.5 * ((fields[1, x + 1] - fields[1, x - 1]) + (next_y(v1) - prev_y(v1))) + fields[3, x]
        b = t * inv
        goal[x] = b
        pa[x] = -b

    def sweep(src, dst, coefs, right, low, high, k):
        xl, xu, yl, yu, zl, zu = coefs
        for x in range(low, high):
            v = src[x]
            t = xl[x] * src[x - 1] + xu[x] * src[x + 1]
            t = t + (yl[x] * prev_y(v, k) + yu[x] * next_y(v, k))
            t = t + (zl[x] * prev_z(v, k) + zu[x] * next_z(v, k))
            dst[x] = (1.0 - damping) * v + (t - right[x])

    fine = (xa, xb, ya, yb, za, zb)
    coarse = (cxa, cxb, cya, cyb, cza, czb)

    def coarse_setup():
        for x in range(1, cw - 1):
            m = coarse_m[x]
            lo_x, hi_x = 0.5 * (m + coarse_m[x - 1]), 0.5 * (m + coarse_m[x + 1])
            lo_y, hi_y = 0.5 * (m + prev_y(m, 2)), 0.5 * (m + next_y(m, 2))
            lo_z = 0.5 * (m + jnp.where(lane_w < 2, 0.0, prev_z(m, 2)))
            hi_z = 0.5 * (m + jnp.where(lane_w >= cells_z - 2, 0.0, next_z(m, 2)))
            diag = lo_x + hi_x + lo_y + hi_y + lo_z + hi_z
            inside = m > 0.0
            inv = jnp.where(inside, damping / jnp.where(inside, diag, 1.0), 0.0)
            cxa[x], cxb[x] = lo_x * inv, hi_x * inv
            cya[x], cyb[x] = lo_y * inv, hi_y * inv
            cza[x] = jnp.where(lane_w < 2, 0.0, lo_z * inv)
            czb[x] = jnp.where(lane_w >= cells_z - 2, 0.0, hi_z * inv)
            if 2 * half <= x < 3 * half:
                cinv[x - 2 * half] = inv[HY : HY + cells_y]

    def correct(at, pre):
        if at == 0:
            m_x[1]()
            coarse_setup()
        for c in range(half):
            r = None
            for x in (HX + 2 * c, HX + 2 * c + 1):
                v = pre[x]
                t = xa[x] * pre[x - 1] + xb[x] * pre[x + 1]
                t = t + (ya[x] * prev_y(v) + yb[x] * next_y(v))
                t = t + (za[x] * prev_z(v) + zb[x] * next_z(v))
                d = (damping * v - (t - goal[x]))[HY : HY + cells_y] * scale_back[x - HX]
                r = d if r is None else r + d
            rhs[at, 2 * half + c, own_y] = 0.5 * pair_sum(r, row_o, lane_o) * cinv[c]
        r_x[at][0]()
        r_x[at][1]()
        right = rhs.at[at]
        for x in range(cw):
            ca[x] = -right[x]
        src, dst = ca, cb
        for step in range(1, COARSE):
            sweep(src, dst, coarse, right, step, cw - step, 2)
            src, dst = dst, src
        other = pb if pre is pa else pa
        for x in range(2, wx - 2):
            pre[x] = pre[x] + src[2 * half + (x - HX) // 2]
        sweep(pre, other, fine, goal, 3, wx - 3, 1)
        sweep(other, pre, fine, goal, HX, HX + cells_x, 1)

    sweep(pa, pb, fine, goal, 2, wx - 2, 1)
    correct(0, pb)
    for x in range(HX, HX + cells_x):
        press[x, own_y] = pb[x, own_y]
    p_x[0]()
    p_x[1]()
    sweep(press, pa, fine, goal, 1, wx - 1, 1)
    sweep(pa, pb, fine, goal, 2, wx - 2, 1)
    correct(1, pb)
    for x in range(HX, HX + cells_x):
        v = pb[x, own_y]
        last[x, own_y] = v
        pres_out[x - HX] = v
    l_x[0]()
    s_x[1]()
    l_x[1]()

    mid = slice(HY, HY + cells_y)
    move_x = []
    for x in range(HX - 1, HX + cells_x + 1):
        grad = 0.5 * (last[x + 1, own_y] - last[x - 1, own_y])
        move_x.append(fields[1, x, own_y] - fields[0, x, own_y] * grad)
    for x in range(cells_x):
        w = x + HX
        v = last[w]
        move_y = fields[2, w] - fields[0, w] * (0.5 * (next_y(v) - prev_y(v)))
        own = v[mid]
        dz = jnp.where(lane_o == cells_z - 1, 0.0, next_z(own)) - jnp.where(lane_o == 0, 0.0, prev_z(own))
        move_z = velocity[2, x] - fields[0, w, own_y] * (0.5 * dz)
        vel_out[0, x] = move_x[x + 1]
        vel_out[1, x] = move_y[mid]
        vel_out[2, x] = move_z
        lo_x, hi_x = 0.5 * (move_x[x] + move_x[x + 1]), 0.5 * (move_x[x + 1] + move_x[x + 2])
        lo_y, hi_y = (0.5 * (move_y + prev_y(move_y)))[mid], (0.5 * (move_y + next_y(move_y)))[mid]
        lo_z = 0.5 * (move_z + jnp.where(lane_o == 0, 0.0, prev_z(move_z)))
        hi_z = 0.5 * (move_z + jnp.where(lane_o == cells_z - 1, 0.0, next_z(move_z)))

        def into(flow):
            return time_step * jnp.maximum(flow, 0.0)

        def back(flow):
            return -time_step * jnp.minimum(flow, 0.0)

        keep = 1.0 - (into(hi_x) + into(hi_y) + into(hi_z)) - (back(lo_x) + back(lo_y) + back(lo_z))
        from_xl, from_xu = into(lo_x), back(hi_x)
        from_yl, from_yu = into(lo_y), back(hi_y)
        from_zl = jnp.where(lane_o == 0, 0.0, into(lo_z))
        from_zu = jnp.where(lane_o == cells_z - 1, 0.0, back(hi_z))
        for s in range(species.shape[0]):
            q = species[s, x]
            xl = rim_x[0, s] if x == 0 else species[s, x - 1]
            xu = rim_x[1, s] if x == cells_x - 1 else species[s, x + 1]
            yl = jnp.where(row_o == 0, rim_y[0, s, x, 0:1], prev_y(q))
            yu = jnp.where(row_o == cells_y - 1, rim_y[1, s, x, 0:1], next_y(q))
            total = keep * q + (from_xl * xl + from_xu * xu) + (from_yl * yl + from_yu * yu)
            spec_out[s, x] = total + (from_zl * prev_z(q) + from_zu * next_z(q))

    for x in (f_x, m_x, s_x, r_x[0], p_x, r_x[1], l_x):
        x[2]()


def local(slabs, crosses, velocity, density, source, species):
    cells_x, cells_y, cells_z = density.shape
    assert cells_x == HX and cells_y % HY == 0
    wx, wy = cells_x + 2 * HX, cells_y + 2 * HY
    cw = 5 * cells_x // 2
    kinds = species.shape[0]
    f32 = jnp.float32

    def vmem(*shape):
        return pltpu.VMEM(shape, f32)

    fine, coarse = vmem(wx, wy, cells_z), vmem(cw, wy, cells_z)
    near, wide, side = (pltpu.SemaphoreType.DMA((len(d),)) for d in (NEAR, WIDE, SIDE))
    both = pltpu.SemaphoreType.DMA((CYCLES, len(WIDE)))
    spec = pl.BlockSpec(memory_space=pltpu.VMEM)
    return pl.pallas_call(
        functools.partial(kernel, slabs, crosses),
        out_shape=tuple(jax.ShapeDtypeStruct(a.shape, f32) for a in (velocity, density, species)),
        in_specs=[spec] * 4,
        out_specs=(spec,) * 3,
        scratch_shapes=[
            vmem(4, wx, wy, cells_z), coarse, vmem(CYCLES, cw, wy, cells_z), fine,
            vmem(2, kinds, cells_y, cells_z), vmem(2, kinds, cells_x, 8, cells_z), fine,
            fine, fine, fine, fine, fine, fine, fine, vmem(cells_x, cells_y, cells_z), fine, fine,
            coarse, coarse, coarse, coarse, coarse, coarse, vmem(cells_x // 2, cells_y, cells_z), coarse, coarse,
            near, near, wide, wide, both, both, near, near, side, side, side, side,
        ],
        compiler_params=pltpu.CompilerParams(collective_id=0, has_side_effects=True),
        name="projection",
    )(velocity, density, source, species)


def solution(mesh):
    plane, stack = P("slab", "cross", None), P(None, "slab", "cross", None)
    return jax.shard_map(
        functools.partial(local, mesh.shape["slab"], mesh.shape["cross"]),
        mesh=mesh,
        in_specs=(stack, plane, plane, stack),
        out_specs=(stack, plane, stack),
        check_vma=False,
    )
```

```python
import functools

import jax
import jax.numpy as jnp
from jax import lax
from jax.experimental import pallas as pl
from jax.experimental.pallas import tpu as pltpu
from jax.sharding import PartitionSpec as P

CYCLES = 2
COARSE = 4
damping = 0.8
time_step = 0.25
MESH = pl.DeviceIdType.MESH
RX = 5
RY = 8
CX = 6
CY = 12

NEAR = [(dx, dy) for dx in (-1, 0, 1) for dy in (-1, 0, 1) if (dx, dy) != (0, 0)] + [(-2, 0), (2, 0)]
WIDE = [(dx, dy) for dx in range(-3, 4) for dy in (-1, 0, 1) if (dx, dy) != (0, 0)]
SIDE = [(-1, 0), (1, 0), (0, -1), (0, 1)]
HX, HY = RX, RY


def kernel(
    slabs, crosses, velocity_in, density_in, source_in, species,
    out_x, out_y, out_z, out_p, rim_x, rim_y,
    velocity, density, source, fields, coarse_m, rhs, press,
    xa, xb, ya, yb, za, zb, goal, scale_back, pa, pb,
    cxa, cxb, cya, cyb, cza, czb, cinv, ca, cb, in_sem,
    f_send, f_recv, m_send, m_recv, r_send, r_recv, p_send, p_recv, s_send, s_recv,
):
    cells_x, cells_y, cells_z = density.shape
    wx, wy = cells_x + 2 * HX, cells_y + 2 * HY
    half = cells_x // 2
    cw, cy = half + 2 * CX, cells_y + 2 * CY
    own_y = pl.ds(HY, cells_y)
    own_x = pl.ds(HX, cells_x)
    own_c = pl.ds(CX, half)
    own_cy = pl.ds(CY, cells_y)
    slab, cross = lax.axis_index("slab"), lax.axis_index("cross")
    f32 = jnp.float32

    def there(dx, dy):
        return (slab + dx >= 0) & (slab + dx < slabs) & (cross + dy >= 0) & (cross + dy < crosses)

    def ys(dy, k, rim):
        if dy == 0:
            return pl.ds(rim, cells_y), pl.ds(rim, cells_y)
        if dy > 0:
            return pl.ds(rim + cells_y - k, k), pl.ds(rim - k, k)
        return pl.ds(rim, k), pl.ds(rim + cells_y, k)

    def fine_cut(dx, dy):
        step = max(0, (abs(dx) - 1) * cells_x + 1) if dx != 0 else 0
        k = RX - step
        sy, dyy = ys(dy, k, HY)
        depth = min(cells_x, RX + 1 - step) if dx != 0 else cells_x
        if dx == 0:
            sx, dst_x = own_x, own_x
        elif dx > 0:
            sx, dst_x = pl.ds(HX + cells_x - depth, depth), pl.ds(HX + (1 - dx) * cells_x - depth, depth)
        else:
            sx, dst_x = pl.ds(HX, depth), pl.ds(HX - dx * cells_x, depth)
        return (sx, sy), (dst_x, dyy)

    def coarse_cut(dx, dy):
        step = (abs(dx) - 1) * half + 1 if dx != 0 else 0
        sy, dyy = ys(dy, 2 * (CX - step), CY)
        return (own_c, sy), (pl.ds(CX - dx * half, half), dyy)

    def within(cut, ref, *lead):
        def both(dx, dy):
            src, dst = cut(dx, dy)
            return ref.at[lead + src], ref.at[lead + dst]

        return both

    def exchange(directions, cut, send, recv):
        def copy(index, dx, dy):
            src, dst = cut(dx, dy)
            return pltpu.make_async_remote_copy(
                src_ref=src, dst_ref=dst, send_sem=send.at[index], recv_sem=recv.at[index],
                device_id=(slab + dx, cross + dy), device_id_type=MESH,
            )

        def start():
            for index, (dx, dy) in enumerate(directions):
                @pl.when(there(dx, dy))
                def _():
                    copy(index, dx, dy).start()

        def arrive():
            for index, (dx, dy) in enumerate(directions):
                @pl.when(there(-dx, -dy))
                def _():
                    copy(index, dx, dy).wait_recv()

        def leave():
            for index, (dx, dy) in enumerate(directions):
                @pl.when(there(dx, dy))
                def _():
                    copy(index, dx, dy).wait_send()

        return start, arrive, leave

    f_x = exchange(NEAR, within(fine_cut, fields, slice(None)), f_send, f_recv)
    m_x = exchange(WIDE, within(coarse_cut, coarse_m), m_send, m_recv)
    r_x = [exchange(WIDE, within(coarse_cut, rhs, at), r_send.at[at], r_recv.at[at]) for at in range(CYCLES)]
    p_x = [exchange(NEAR, within(fine_cut, press, at), p_send.at[at], p_recv.at[at]) for at in range(CYCLES)]

    def species_cut(dx, dy):
        if dx != 0:
            return species.at[:, cells_x - 1 if dx > 0 else 0], rim_x.at[0 if dx > 0 else 1]
        return species.at[:, :, cells_y - 1 if dy > 0 else 0], rim_y.at[0 if dy > 0 else 1]

    s_x = exchange(SIDE, species_cut, s_send, s_recv)

    def grids(rows):
        lane = lax.broadcasted_iota(jnp.int32, (rows, cells_z), 1)
        row = lax.broadcasted_iota(jnp.int32, (rows, cells_z), 0)
        return row, lane

    def next_z(v, k=1):
        return pltpu.roll(v, cells_z - k, 1)

    def prev_z(v, k=1):
        return pltpu.roll(v, k, 1)

    def next_y(v, k=1):
        return pltpu.roll(v, v.shape[0] - k, 0)

    def prev_y(v, k=1):
        return pltpu.roll(v, k, 0)

    row_w, lane_w = grids(wy)
    row_c, lane_c = grids(cy)
    row_o, lane_o = grids(cells_y)

    def pair_sum(v, row, lane):
        v = v + jnp.where(row % 2 == 0, next_y(v), prev_y(v))
        return v + jnp.where(lane % 2 == 0, next_z(v), prev_z(v))

    inputs = [
        pltpu.make_async_copy(src, dst, in_sem.at[at])
        for at, (src, dst) in enumerate(((velocity_in, velocity), (density_in, density), (source_in, source)))
    ]
    for copy in inputs:
        copy.start()
    for ref in (fields, coarse_m, rhs, press, rim_x, rim_y):
        ref[...] = jnp.zeros(ref.shape, f32)
    barrier = pltpu.get_barrier_semaphore()
    count = jnp.int32(0)
    for dx, dy in WIDE:
        here = there(dx, dy)
        count = count + here.astype(jnp.int32)

        @pl.when(here)
        def _():
            pl.semaphore_signal(barrier, inc=1, device_id=(slab + dx, cross + dy), device_id_type=MESH)

    for copy in inputs:
        copy.wait()
    for x in range(cells_x):
        v2 = velocity[2, x]
        dz = jnp.where(lane_o == cells_z - 1, 0.0, next_z(v2)) - jnp.where(lane_o == 0, 0.0, prev_z(v2))
        fields[0, HX + x, own_y] = 1.0 / density[x]
        fields[1, HX + x, own_y] = velocity[0, x]
        fields[2, HX + x, own_y] = velocity[1, x]
        fields[3, HX + x, own_y] = 0.5 * dz - source[x]
    for c in range(half):
        m = 1.0 / density[2 * c] + 1.0 / density[2 * c + 1]
        coarse_m[CX + c, own_cy] = 0.125 * pair_sum(m, row_o, lane_o)
    pl.semaphore_wait(barrier, count)
    f_x[0]()
    m_x[0]()
    s_x[0]()
    f_x[1]()

    for x in range(1, wx - 1):
        m = fields[0, x]
        lo_x, hi_x = 0.5 * (m + fields[0, x - 1]), 0.5 * (m + fields[0, x + 1])
        lo_y, hi_y = 0.5 * (m + prev_y(m)), 0.5 * (m + next_y(m))
        lo_z = 0.5 * (m + jnp.where(lane_w == 0, 0.0, prev_z(m)))
        hi_z = 0.5 * (m + jnp.where(lane_w == cells_z - 1, 0.0, next_z(m)))
        diag = lo_x + hi_x + lo_y + hi_y + lo_z + hi_z
        inside = m > 0.0
        inv = jnp.where(inside, damping / jnp.where(inside, diag, 1.0), 0.0)
        xa[x], xb[x] = lo_x * inv, hi_x * inv
        ya[x], yb[x] = lo_y * inv, hi_y * inv
        za[x] = jnp.where(lane_w == 0, 0.0, lo_z * inv)
        zb[x] = jnp.where(lane_w == cells_z - 1, 0.0, hi_z * inv)
        if HX <= x < HX + cells_x:
            scale_back[x - HX] = (diag * (1.0 / damping))[HY : HY + cells_y]
        v1 = fields[2, x]
        t = 0.5 * ((fields[1, x + 1] - fields[1, x - 1]) + (next_y(v1) - prev_y(v1))) + fields[3, x]
        b = t * inv
        goal[x] = b
        pa[x] = -b

    def sweep(src, dst, coefs, right, low, high, k):
        xl, xu, yl, yu, zl, zu = coefs
        for x in range(low, high):
            v = src[x]
            t = xl[x] * src[x - 1] + xu[x] * src[x + 1]
            t = t + (yl[x] * prev_y(v, k) + yu[x] * next_y(v, k))
            t = t + (zl[x] * prev_z(v, k) + zu[x] * next_z(v, k))
            dst[x] = (1.0 - damping) * v + (t - right[x])

    fine = (xa, xb, ya, yb, za, zb)
    coarse = (cxa, cxb, cya, cyb, cza, czb)

    def coarse_setup():
        for x in range(1, cw - 1):
            m = coarse_m[x]
            lo_x, hi_x = 0.5 * (m + coarse_m[x - 1]), 0.5 * (m + coarse_m[x + 1])
            lo_y, hi_y = 0.5 * (m + prev_y(m, 2)), 0.5 * (m + next_y(m, 2))
            lo_z = 0.5 * (m + jnp.where(lane_c < 2, 0.0, prev_z(m, 2)))
            hi_z = 0.5 * (m + jnp.where(lane_c >= cells_z - 2, 0.0, next_z(m, 2)))
            diag = lo_x + hi_x + lo_y + hi_y + lo_z + hi_z
            inside = m > 0.0
            inv = jnp.where(inside, damping / jnp.where(inside, diag, 1.0), 0.0)
            cxa[x], cxb[x] = lo_x * inv, hi_x * inv
            cya[x], cyb[x] = lo_y * inv, hi_y * inv
            cza[x] = jnp.where(lane_c < 2, 0.0, lo_z * inv)
            czb[x] = jnp.where(lane_c >= cells_z - 2, 0.0, hi_z * inv)
            if CX <= x < CX + half:
                cinv[x - CX] = inv[CY : CY + cells_y]

    def correct(at, pre, free, reach):
        for x in range(HX, HX + cells_x):
            press[at, x, own_y] = pre[x, own_y]
        p_x[at][0]()
        if at == 0:
            m_x[1]()
            coarse_setup()
        for c in range(half):
            r = None
            for x in (HX + 2 * c, HX + 2 * c + 1):
                v = pre[x]
                t = xa[x] * pre[x - 1] + xb[x] * pre[x + 1]
                t = t + (ya[x] * prev_y(v) + yb[x] * next_y(v))
                t = t + (za[x] * prev_z(v) + zb[x] * next_z(v))
                d = (damping * v - (t - goal[x]))[HY : HY + cells_y] * scale_back[x - HX]
                r = d if r is None else r + d
            rhs[at, CX + c, own_cy] = 0.5 * pair_sum(r, row_o, lane_o) * cinv[c]
        r_x[at][0]()
        r_x[at][1]()
        right = rhs.at[at]
        for x in range(cw):
            ca[x] = -right[x]
        src, dst = ca, cb
        for step in range(1, COARSE):
            sweep(src, dst, coarse, right, step, cw - step, 2)
            src, dst = dst, src
        p_x[at][1]()
        low, high = HX - reach - 2, HX + cells_x + reach + 2
        for x in range(low, high):
            pre[x] = press[at, x] + src[CX + (x - HX) // 2, pl.ds(CY - HY, wy)]
        sweep(pre, free, fine, goal, low + 1, high - 1, 1)
        sweep(free, pre, fine, goal, low + 2, high - 2, 1)

    sweep(pa, pb, fine, goal, HX - 1, HX + cells_x + 1, 1)
    correct(0, pb, pa, 3)
    sweep(pb, pa, fine, goal, HX - 2, HX + cells_x + 2, 1)
    sweep(pa, pb, fine, goal, HX - 1, HX + cells_x + 1, 1)
    correct(1, pb, pa, 2)
    last = pb

    for x in range(HX - 1, HX + cells_x + 1):
        grad = 0.5 * (last[x + 1, own_y] - last[x - 1, own_y])
        out_x[x - HX + 1] = fields[1, x, own_y] - fields[0, x, own_y] * grad
    for x in range(cells_x):
        w = x + HX
        v = last[w]
        out_y[x] = fields[2, w] - fields[0, w] * (0.5 * (next_y(v) - prev_y(v)))
        own = v[HY : HY + cells_y]
        dz = jnp.where(lane_o == cells_z - 1, 0.0, next_z(own)) - jnp.where(lane_o == 0, 0.0, prev_z(own))
        out_z[x] = velocity[2, x] - fields[0, w, own_y] * (0.5 * dz)
        out_p[x] = own
    s_x[1]()
    for x in (f_x, m_x, s_x, *r_x, *p_x):
        x[2]()


def transport(in_x, in_y, in_z, in_p, rim_x, rim_y, species, vel_out, pres_out, spec_out):
    cells_x, cells_y, cells_z = in_p.shape
    lane_o = lax.broadcasted_iota(jnp.int32, (cells_y, cells_z), 1)
    row_o = lax.broadcasted_iota(jnp.int32, (cells_y, cells_z), 0)

    def next_z(v):
        return pltpu.roll(v, cells_z - 1, 1)

    def prev_z(v):
        return pltpu.roll(v, 1, 1)

    def next_y(v):
        return pltpu.roll(v, v.shape[0] - 1, 0)

    def prev_y(v):
        return pltpu.roll(v, 1, 0)

    mid = slice(HY, HY + cells_y)
    pres_out[...] = in_p[...]
    move_x = [in_x[x] for x in range(cells_x + 2)]
    for x in range(cells_x):
        move_y, move_z = in_y[x], in_z[x]
        vel_out[0, x] = move_x[x + 1]
        vel_out[1, x] = move_y[mid]
        vel_out[2, x] = move_z
        lo_x, hi_x = 0.5 * (move_x[x] + move_x[x + 1]), 0.5 * (move_x[x + 1] + move_x[x + 2])
        lo_y, hi_y = (0.5 * (move_y + prev_y(move_y)))[mid], (0.5 * (move_y + next_y(move_y)))[mid]
        lo_z = 0.5 * (move_z + jnp.where(lane_o == 0, 0.0, prev_z(move_z)))
        hi_z = 0.5 * (move_z + jnp.where(lane_o == cells_z - 1, 0.0, next_z(move_z)))

        def into(flow):
            return time_step * jnp.maximum(flow, 0.0)

        def back(flow):
            return -time_step * jnp.minimum(flow, 0.0)

        keep = 1.0 - (into(hi_x) + into(hi_y) + into(hi_z)) - (back(lo_x) + back(lo_y) + back(lo_z))
        from_xl, from_xu = into(lo_x), back(hi_x)
        from_yl, from_yu = into(lo_y), back(hi_y)
        from_zl = jnp.where(lane_o == 0, 0.0, into(lo_z))
        from_zu = jnp.where(lane_o == cells_z - 1, 0.0, back(hi_z))
        for s in range(species.shape[0]):
            q = species[s, x]
            xl = rim_x[0, s] if x == 0 else species[s, x - 1]
            xu = rim_x[1, s] if x == cells_x - 1 else species[s, x + 1]
            yl = jnp.where(row_o == 0, rim_y[0, s, pl.ds(x, 1)], prev_y(q))
            yu = jnp.where(row_o == cells_y - 1, rim_y[1, s, pl.ds(x, 1)], next_y(q))
            total = keep * q + (from_xl * xl + from_xu * xu) + (from_yl * yl + from_yu * yu)
            spec_out[s, x] = total + (from_zl * prev_z(q) + from_zu * next_z(q))


def local(slabs, crosses, velocity, density, source, species):
    cells_x, cells_y, cells_z = density.shape
    assert cells_x == 4 and cells_y % 8 == 0 and cells_y >= CY
    wx, wy = cells_x + 2 * HX, cells_y + 2 * HY
    half = cells_x // 2
    kinds = species.shape[0]
    f32 = jnp.float32

    def vmem(*shape):
        return pltpu.VMEM(shape, f32)

    fine, coarse = (wx, wy, cells_z), (half + 2 * CX, cells_y + 2 * CY, cells_z)
    near, wide, side = len(NEAR), len(WIDE), len(SIDE)
    dma = pltpu.SemaphoreType.DMA
    spec = pl.BlockSpec(memory_space=pltpu.VMEM)
    anywhere = pl.BlockSpec(memory_space=pl.ANY)
    moved = [
        (cells_x + 2, cells_y, cells_z), (cells_x, wy, cells_z), density.shape, density.shape,
        (2, kinds, cells_y, cells_z), (2, kinds, cells_x, cells_z),
    ]
    between = pl.pallas_call(
        functools.partial(kernel, slabs, crosses),
        out_shape=tuple(jax.ShapeDtypeStruct(shape, f32) for shape in moved),
        in_specs=[anywhere] * 4,
        out_specs=(spec,) * 6,
        scratch_shapes=[vmem(*velocity.shape), vmem(*density.shape), vmem(*density.shape)]
        + [vmem(4, *fine), vmem(*coarse), vmem(CYCLES, *coarse), vmem(CYCLES, *fine)]
        + [vmem(*fine)] * 7 + [vmem(*density.shape)] + [vmem(*fine)] * 2
        + [vmem(*coarse)] * 6 + [vmem(half, cells_y, cells_z)] + [vmem(*coarse)] * 2
        + [dma((3,))] + [dma((near,))] * 2 + [dma((wide,))] * 2
        + [dma((CYCLES, wide))] * 2 + [dma((CYCLES, near))] * 2 + [dma((side,))] * 2,
        compiler_params=pltpu.CompilerParams(collective_id=0, has_side_effects=True),
        name="projection",
    )(velocity, density, source, species)
    return pl.pallas_call(
        transport,
        out_shape=tuple(jax.ShapeDtypeStruct(a.shape, f32) for a in (velocity, density, species)),
        in_specs=[spec] * 7,
        out_specs=(spec,) * 3,
        name="transport",
    )(*between, species)


def solution(mesh):
    plane, stack = P("slab", "cross", None), P(None, "slab", "cross", None)
    return jax.shard_map(
        functools.partial(local, mesh.shape["slab"], mesh.shape["cross"]),
        mesh=mesh,
        in_specs=(stack, plane, plane, stack),
        out_specs=(stack, plane, stack),
        check_vma=False,
    )
```

```python
import functools

import jax
import jax.numpy as jnp
from jax import lax
from jax.experimental import pallas as pl
from jax.experimental.pallas import tpu as pltpu
from jax.sharding import PartitionSpec as P

CYCLES = 2
COARSE = 4
damping = 0.8
time_step = 0.25
MESH = pl.DeviceIdType.MESH
RX = 5
RY = 8
CX = 6
CY = 12

NEAR = [(dx, dy) for dx in (-1, 0, 1) for dy in (-1, 0, 1) if (dx, dy) != (0, 0)] + [(-2, 0), (2, 0)]
WIDE = [(dx, dy) for dx in range(-3, 4) for dy in (-1, 0, 1) if (dx, dy) != (0, 0)]
SIDE = [(-1, 0), (1, 0), (0, -1), (0, 1)]
HX, HY = RX, RY


def kernel(
    slabs, crosses, velocity_in, density_in, source_in, species,
    out_x, out_y, out_z, out_p, rim_x, rim_y,
    velocity, density, source, fields, packed_m, packed_r, press, coarse_m, right,
    xa, xb, ya, yb, za, zb, goal, scale_back, pa, pb,
    cxa, cxb, cya, cyb, cza, czb, cinv, ca, cb, in_sem,
    f_send, f_recv, m_send, m_recv, r_send, r_recv, p_send, p_recv, s_send, s_recv,
):
    cells_x, cells_y, cells_z = density.shape
    wx, wy = cells_x + 2 * HX, cells_y + 2 * HY
    half = cells_x // 2
    cw, cy = half + 2 * CX, cells_y + 2 * CY
    own_y = pl.ds(HY, cells_y)
    own_x = pl.ds(HX, cells_x)
    own_cy = pl.ds(CY, cells_y)
    slab, cross = lax.axis_index("slab"), lax.axis_index("cross")
    f32 = jnp.float32

    def there(dx, dy):
        return (slab + dx >= 0) & (slab + dx < slabs) & (cross + dy >= 0) & (cross + dy < crosses)

    def ys(dy, k, rim):
        if dy == 0:
            return pl.ds(rim, cells_y), pl.ds(rim, cells_y)
        if dy > 0:
            return pl.ds(rim + cells_y - k, k), pl.ds(rim - k, k)
        return pl.ds(rim, k), pl.ds(rim + cells_y, k)

    def fine_cut(dx, dy):
        step = max(0, (abs(dx) - 1) * cells_x + 1) if dx != 0 else 0
        k = RX - step
        sy, dyy = ys(dy, k, HY)
        depth = min(cells_x, RX + 1 - step) if dx != 0 else cells_x
        if dx == 0:
            sx, dst_x = own_x, own_x
        elif dx > 0:
            sx, dst_x = pl.ds(HX + cells_x - depth, depth), pl.ds(HX + (1 - dx) * cells_x - depth, depth)
        else:
            sx, dst_x = pl.ds(HX, depth), pl.ds(HX - dx * cells_x, depth)
        return (sx, sy), (dst_x, dyy)

    def coarse_cut(dx, dy):
        step = (abs(dx) - 1) * half + 1 if dx != 0 else 0
        sy, dyy = ys(dy, 2 * (CX - step), CY)
        return (CX // half, sy), (CX // half - dx, dyy)

    def within(cut, ref, *lead):
        def both(dx, dy):
            src, dst = cut(dx, dy)
            return ref.at[lead + src], ref.at[lead + dst]

        return both

    def exchange(directions, cut, send, recv):
        def copy(index, dx, dy):
            src, dst = cut(dx, dy)
            return pltpu.make_async_remote_copy(
                src_ref=src, dst_ref=dst, send_sem=send.at[index], recv_sem=recv.at[index],
                device_id=(slab + dx, cross + dy), device_id_type=MESH,
            )

        def start():
            for index, (dx, dy) in enumerate(directions):
                @pl.when(there(dx, dy))
                def _():
                    copy(index, dx, dy).start()

        def arrive():
            for index, (dx, dy) in enumerate(directions):
                @pl.when(there(-dx, -dy))
                def _():
                    copy(index, dx, dy).wait_recv()

        def leave():
            for index, (dx, dy) in enumerate(directions):
                @pl.when(there(dx, dy))
                def _():
                    copy(index, dx, dy).wait_send()

        return start, arrive, leave

    def fields_cut(dx, dy):
        return within(fine_cut, fields, slice(0, 2) if abs(dx) > 1 else slice(None))(dx, dy)

    f_x = exchange(NEAR, fields_cut, f_send, f_recv)
    m_x = exchange(WIDE, within(coarse_cut, packed_m), m_send, m_recv)
    r_x = [exchange(WIDE, within(coarse_cut, packed_r, at), r_send.at[at], r_recv.at[at]) for at in range(CYCLES)]
    p_x = [exchange(NEAR, within(fine_cut, press, at), p_send.at[at], p_recv.at[at]) for at in range(CYCLES)]

    def species_cut(dx, dy):
        if dx != 0:
            return species.at[:, cells_x - 1 if dx > 0 else 0], rim_x.at[0 if dx > 0 else 1]
        return species.at[:, :, cells_y - 1 if dy > 0 else 0], rim_y.at[0 if dy > 0 else 1]

    s_x = exchange(SIDE, species_cut, s_send, s_recv)

    def grids(rows):
        lane = lax.broadcasted_iota(jnp.int32, (rows, cells_z), 1)
        row = lax.broadcasted_iota(jnp.int32, (rows, cells_z), 0)
        return row, lane

    def next_z(v, k=1):
        return pltpu.roll(v, cells_z - k, 1)

    def prev_z(v, k=1):
        return pltpu.roll(v, k, 1)

    def next_y(v, k=1):
        return pltpu.roll(v, v.shape[0] - k, 0)

    def prev_y(v, k=1):
        return pltpu.roll(v, k, 0)

    row_w, lane_w = grids(wy)
    row_c, lane_c = grids(cy)
    row_o, lane_o = grids(cells_y)

    def pair_sum(v, row, lane):
        v = v + jnp.where(row % 2 == 0, next_y(v), prev_y(v))
        return v + jnp.where(lane % 2 == 0, next_z(v), prev_z(v))

    def pack(two):
        return jnp.where(lane_o % 2 == 0, two[0], two[1])

    def unpack(ref, dst):
        for block in range(2 * CX // half + 1):
            e = ref[block]
            dst[2 * block] = jnp.where(lane_c % 2 == 0, e, prev_z(e))
            dst[2 * block + 1] = jnp.where(lane_c % 2 == 0, next_z(e), e)

    inputs = [
        pltpu.make_async_copy(src, dst, in_sem.at[at])
        for at, (src, dst) in enumerate(((velocity_in, velocity), (density_in, density), (source_in, source)))
    ]
    for copy in inputs:
        copy.start()
    for ref in (fields, packed_m, packed_r, press, rim_x, rim_y):
        ref[...] = jnp.zeros(ref.shape, f32)
    barrier = pltpu.get_barrier_semaphore()
    count = jnp.int32(0)
    for dx, dy in WIDE:
        here = there(dx, dy)
        count = count + here.astype(jnp.int32)

        @pl.when(here)
        def _():
            pl.semaphore_signal(barrier, inc=1, device_id=(slab + dx, cross + dy), device_id_type=MESH)

    for copy in inputs:
        copy.wait()
    for x in range(cells_x):
        v2 = velocity[2, x]
        dz = jnp.where(lane_o == cells_z - 1, 0.0, next_z(v2)) - jnp.where(lane_o == 0, 0.0, prev_z(v2))
        fields[0, HX + x, own_y] = 1.0 / density[x]
        fields[1, HX + x, own_y] = velocity[0, x]
        fields[2, HX + x, own_y] = velocity[1, x]
        fields[3, HX + x, own_y] = 0.5 * dz - source[x]
    means = []
    for c in range(half):
        m = 1.0 / density[2 * c] + 1.0 / density[2 * c + 1]
        means.append(0.125 * pair_sum(m, row_o, lane_o))
    packed_m[CX // half, own_cy] = pack(means)
    pl.semaphore_wait(barrier, count)
    f_x[0]()
    m_x[0]()
    s_x[0]()
    f_x[1]()

    def fine_setup(rows):
        for x in rows:
            m = fields[0, x]
            lo_x, hi_x = 0.5 * (m + fields[0, x - 1]), 0.5 * (m + fields[0, x + 1])
            lo_y, hi_y = 0.5 * (m + prev_y(m)), 0.5 * (m + next_y(m))
            lo_z = 0.5 * (m + jnp.where(lane_w == 0, 0.0, prev_z(m)))
            hi_z = 0.5 * (m + jnp.where(lane_w == cells_z - 1, 0.0, next_z(m)))
            diag = lo_x + hi_x + lo_y + hi_y + lo_z + hi_z
            inside = m > 0.0
            inv = jnp.where(inside, damping / jnp.where(inside, diag, 1.0), 0.0)
            xa[x], xb[x] = lo_x * inv, hi_x * inv
            ya[x], yb[x] = lo_y * inv, hi_y * inv
            za[x] = jnp.where(lane_w == 0, 0.0, lo_z * inv)
            zb[x] = jnp.where(lane_w == cells_z - 1, 0.0, hi_z * inv)
            if HX <= x < HX + cells_x:
                scale_back[x - HX] = (diag * (1.0 / damping))[HY : HY + cells_y]
            v1 = fields[2, x]
            t = 0.5 * ((fields[1, x + 1] - fields[1, x - 1]) + (next_y(v1) - prev_y(v1))) + fields[3, x]
            b = t * inv
            goal[x] = b
            pa[x] = -b

    early = range(HX - 2, HX + cells_x + 2)
    fine_setup(early)

    def sweep(src, dst, coefs, right, low, high, k):
        xl, xu, yl, yu, zl, zu = coefs
        for x in range(low, high):
            v = src[x]
            t = xl[x] * src[x - 1] + xu[x] * src[x + 1]
            t = t + (yl[x] * prev_y(v, k) + yu[x] * next_y(v, k))
            t = t + (zl[x] * prev_z(v, k) + zu[x] * next_z(v, k))
            dst[x] = (1.0 - damping) * v + (t - right[x])

    fine = (xa, xb, ya, yb, za, zb)
    coarse = (cxa, cxb, cya, cyb, cza, czb)

    def coarse_setup(rows):
        for x in rows:
            m = coarse_m[x]
            lo_x, hi_x = 0.5 * (m + coarse_m[x - 1]), 0.5 * (m + coarse_m[x + 1])
            lo_y, hi_y = 0.5 * (m + prev_y(m, 2)), 0.5 * (m + next_y(m, 2))
            lo_z = 0.5 * (m + jnp.where(lane_c < 2, 0.0, prev_z(m, 2)))
            hi_z = 0.5 * (m + jnp.where(lane_c >= cells_z - 2, 0.0, next_z(m, 2)))
            diag = lo_x + hi_x + lo_y + hi_y + lo_z + hi_z
            inside = m > 0.0
            inv = jnp.where(inside, damping / jnp.where(inside, diag, 1.0), 0.0)
            cxa[x], cxb[x] = lo_x * inv, hi_x * inv
            cya[x], cyb[x] = lo_y * inv, hi_y * inv
            cza[x] = jnp.where(lane_c < 2, 0.0, lo_z * inv)
            czb[x] = jnp.where(lane_c >= cells_z - 2, 0.0, hi_z * inv)
            if CX <= x < CX + half:
                cinv[x - CX] = inv[CY : CY + cells_y]

    def correct(at, pre, free, reach):
        for x in range(HX, HX + cells_x):
            press[at, x, own_y] = pre[x, own_y]
        own_rows = range(CX, CX + half)
        if at == 0:
            m_x[1]()
            unpack(packed_m, coarse_m)
            coarse_setup(own_rows)
        sums = []
        for c in range(half):
            r = None
            for x in (HX + 2 * c, HX + 2 * c + 1):
                v = pre[x]
                t = xa[x] * pre[x - 1] + xb[x] * pre[x + 1]
                t = t + (ya[x] * prev_y(v) + yb[x] * next_y(v))
                t = t + (za[x] * prev_z(v) + zb[x] * next_z(v))
                d = (damping * v - (t - goal[x]))[HY : HY + cells_y] * scale_back[x - HX]
                r = d if r is None else r + d
            sums.append(0.5 * pair_sum(r, row_o, lane_o) * cinv[c])
        packed_r[at, CX // half, own_cy] = pack(sums)
        r_x[at][0]()
        p_x[at][0]()
        if at == 0:
            coarse_setup([x for x in range(1, cw - 1) if x not in own_rows])
            fine_setup([x for x in range(1, wx - 1) if x not in early])
        r_x[at][1]()
        unpack(packed_r.at[at], right)
        for x in range(cw):
            ca[x] = -right[x]
        src, dst = ca, cb
        for step in range(1, COARSE):
            sweep(src, dst, coarse, right, step, cw - step, 2)
            src, dst = dst, src
        p_x[at][1]()
        low, high = HX - reach - 2, HX + cells_x + reach + 2
        for x in range(low, high):
            pre[x] = press[at, x] + src[CX + (x - HX) // 2, pl.ds(CY - HY, wy)]
        sweep(pre, free, fine, goal, low + 1, high - 1, 1)
        sweep(free, pre, fine, goal, low + 2, high - 2, 1)

    sweep(pa, pb, fine, goal, HX - 1, HX + cells_x + 1, 1)
    correct(0, pb, pa, 3)
    sweep(pb, pa, fine, goal, HX - 2, HX + cells_x + 2, 1)
    sweep(pa, pb, fine, goal, HX - 1, HX + cells_x + 1, 1)
    correct(1, pb, pa, 2)
    last = pb

    for x in range(HX - 1, HX + cells_x + 1):
        grad = 0.5 * (last[x + 1, own_y] - last[x - 1, own_y])
        out_x[x - HX + 1] = fields[1, x, own_y] - fields[0, x, own_y] * grad
    for x in range(cells_x):
        w = x + HX
        v = last[w]
        out_y[x] = fields[2, w] - fields[0, w] * (0.5 * (next_y(v) - prev_y(v)))
        own = v[HY : HY + cells_y]
        dz = jnp.where(lane_o == cells_z - 1, 0.0, next_z(own)) - jnp.where(lane_o == 0, 0.0, prev_z(own))
        out_z[x] = velocity[2, x] - fields[0, w, own_y] * (0.5 * dz)
        out_p[x] = own
    s_x[1]()
    for x in (f_x, m_x, s_x, *r_x, *p_x):
        x[2]()


def transport(in_x, in_y, in_z, in_p, rim_x, rim_y, species, vel_out, pres_out, spec_out):
    cells_x, cells_y, cells_z = in_p.shape
    lane_o = lax.broadcasted_iota(jnp.int32, (cells_y, cells_z), 1)
    row_o = lax.broadcasted_iota(jnp.int32, (cells_y, cells_z), 0)

    def next_z(v):
        return pltpu.roll(v, cells_z - 1, 1)

    def prev_z(v):
        return pltpu.roll(v, 1, 1)

    def next_y(v):
        return pltpu.roll(v, v.shape[0] - 1, 0)

    def prev_y(v):
        return pltpu.roll(v, 1, 0)

    mid = slice(HY, HY + cells_y)
    pres_out[...] = in_p[...]
    move_x = [in_x[x] for x in range(cells_x + 2)]
    for x in range(cells_x):
        move_y, move_z = in_y[x], in_z[x]
        vel_out[0, x] = move_x[x + 1]
        vel_out[1, x] = move_y[mid]
        vel_out[2, x] = move_z
        lo_x, hi_x = 0.5 * (move_x[x] + move_x[x + 1]), 0.5 * (move_x[x + 1] + move_x[x + 2])
        lo_y, hi_y = (0.5 * (move_y + prev_y(move_y)))[mid], (0.5 * (move_y + next_y(move_y)))[mid]
        lo_z = 0.5 * (move_z + jnp.where(lane_o == 0, 0.0, prev_z(move_z)))
        hi_z = 0.5 * (move_z + jnp.where(lane_o == cells_z - 1, 0.0, next_z(move_z)))

        def into(flow):
            return time_step * jnp.maximum(flow, 0.0)

        def back(flow):
            return -time_step * jnp.minimum(flow, 0.0)

        keep = 1.0 - (into(hi_x) + into(hi_y) + into(hi_z)) - (back(lo_x) + back(lo_y) + back(lo_z))
        from_xl, from_xu = into(lo_x), back(hi_x)
        from_yl, from_yu = into(lo_y), back(hi_y)
        from_zl = jnp.where(lane_o == 0, 0.0, into(lo_z))
        from_zu = jnp.where(lane_o == cells_z - 1, 0.0, back(hi_z))
        for s in range(species.shape[0]):
            q = species[s, x]
            xl = rim_x[0, s] if x == 0 else species[s, x - 1]
            xu = rim_x[1, s] if x == cells_x - 1 else species[s, x + 1]
            yl = jnp.where(row_o == 0, rim_y[0, s, pl.ds(x, 1)], prev_y(q))
            yu = jnp.where(row_o == cells_y - 1, rim_y[1, s, pl.ds(x, 1)], next_y(q))
            total = keep * q + (from_xl * xl + from_xu * xu) + (from_yl * yl + from_yu * yu)
            spec_out[s, x] = total + (from_zl * prev_z(q) + from_zu * next_z(q))


def local(slabs, crosses, velocity, density, source, species):
    cells_x, cells_y, cells_z = density.shape
    assert cells_x == 4 and CX % (cells_x // 2) == 0 and cells_y % 8 == 0 and cells_y >= CY
    wx, wy = cells_x + 2 * HX, cells_y + 2 * HY
    half = cells_x // 2
    kinds = species.shape[0]
    f32 = jnp.float32

    def vmem(*shape):
        return pltpu.VMEM(shape, f32)

    fine, coarse = (wx, wy, cells_z), (half + 2 * CX, cells_y + 2 * CY, cells_z)
    packed = (2 * CX // half + 1,) + coarse[1:]
    near, wide, side = len(NEAR), len(WIDE), len(SIDE)
    dma = pltpu.SemaphoreType.DMA
    spec = pl.BlockSpec(memory_space=pltpu.VMEM)
    anywhere = pl.BlockSpec(memory_space=pl.ANY)
    moved = [
        (cells_x + 2, cells_y, cells_z), (cells_x, wy, cells_z), density.shape, density.shape,
        (2, kinds, cells_y, cells_z), (2, kinds, cells_x, cells_z),
    ]
    between = pl.pallas_call(
        functools.partial(kernel, slabs, crosses),
        out_shape=tuple(jax.ShapeDtypeStruct(shape, f32) for shape in moved),
        in_specs=[anywhere] * 4,
        out_specs=(spec,) * 6,
        scratch_shapes=[vmem(*velocity.shape), vmem(*density.shape), vmem(*density.shape)]
        + [vmem(4, *fine), vmem(*packed), vmem(CYCLES, *packed), vmem(CYCLES, *fine)]
        + [vmem(*coarse)] * 2
        + [vmem(*fine)] * 7 + [vmem(*density.shape)] + [vmem(*fine)] * 2
        + [vmem(*coarse)] * 6 + [vmem(half, cells_y, cells_z)] + [vmem(*coarse)] * 2
        + [dma((3,))] + [dma((near,))] * 2 + [dma((wide,))] * 2
        + [dma((CYCLES, wide))] * 2 + [dma((CYCLES, near))] * 2 + [dma((side,))] * 2,
        compiler_params=pltpu.CompilerParams(collective_id=0, has_side_effects=True),
        name="projection",
    )(velocity, density, source, species)
    return pl.pallas_call(
        transport,
        out_shape=tuple(jax.ShapeDtypeStruct(a.shape, f32) for a in (velocity, density, species)),
        in_specs=[spec] * 7,
        out_specs=(spec,) * 3,
        name="transport",
    )(*between, species)


def solution(mesh):
    plane, stack = P("slab", "cross", None), P(None, "slab", "cross", None)
    return jax.shard_map(
        functools.partial(local, mesh.shape["slab"], mesh.shape["cross"]),
        mesh=mesh,
        in_specs=(stack, plane, plane, stack),
        out_specs=(stack, plane, stack),
        check_vma=False,
    )
```

```python
import functools

import jax
import jax.numpy as jnp
from jax import lax
from jax.experimental import pallas as pl
from jax.experimental.pallas import tpu as pltpu
from jax.sharding import PartitionSpec as P

CYCLES = 2
COARSE = 4
damping = 0.8
time_step = 0.25
MESH = pl.DeviceIdType.MESH
RX = 5
RY = 8
CX = 6
CY = 12

NEAR = [(dx, dy) for dx in (-1, 0, 1) for dy in (-1, 0, 1) if (dx, dy) != (0, 0)] + [(-2, 0), (2, 0)]
WIDE = [(dx, dy) for dx in range(-3, 4) for dy in (-1, 0, 1) if (dx, dy) != (0, 0)]
SIDE = [(-1, 0), (1, 0), (0, -1), (0, 1)]
HX, HY = RX, RY


def kernel(
    slabs, crosses, velocity_in, density_in, source_in, species,
    out_x, out_y, out_z, out_p, rim_x, rim_y,
    velocity, density, source, fields, packed_m, packed_r, press, coarse_m, right,
    xa, xb, ya, yb, za, zb, goal, scale_back, pa, pb,
    cxa, cxb, cya, cyb, cza, czb, cinv, ca, cb, in_sem,
    f_send, f_recv, m_send, m_recv, r_send, r_recv, p_send, p_recv, s_send, s_recv,
):
    cells_x, cells_y, cells_z = density.shape
    wx, wy = cells_x + 2 * HX, cells_y + 2 * HY
    half = cells_x // 2
    cw, cy = half + 2 * CX, cells_y + 2 * CY
    own_y = pl.ds(HY, cells_y)
    own_x = pl.ds(HX, cells_x)
    own_cy = pl.ds(CY, cells_y)
    slab, cross = lax.axis_index("slab"), lax.axis_index("cross")
    f32 = jnp.float32

    def there(dx, dy):
        return (slab + dx >= 0) & (slab + dx < slabs) & (cross + dy >= 0) & (cross + dy < crosses)

    def ys(dy, k, rim):
        if dy == 0:
            return pl.ds(rim, cells_y), pl.ds(rim, cells_y)
        if dy > 0:
            return pl.ds(rim + cells_y - k, k), pl.ds(rim - k, k)
        return pl.ds(rim, k), pl.ds(rim + cells_y, k)

    def fine_cut(dx, dy):
        step = max(0, (abs(dx) - 1) * cells_x + 1) if dx != 0 else 0
        k = RX - step
        sy, dyy = ys(dy, k, HY)
        depth = min(cells_x, RX + 1 - step) if dx != 0 else cells_x
        if dx == 0:
            sx, dst_x = own_x, own_x
        elif dx > 0:
            sx, dst_x = pl.ds(HX + cells_x - depth, depth), pl.ds(HX + (1 - dx) * cells_x - depth, depth)
        else:
            sx, dst_x = pl.ds(HX, depth), pl.ds(HX - dx * cells_x, depth)
        return (sx, sy), (dst_x, dyy)

    def coarse_cut(dx, dy):
        step = (abs(dx) - 1) * half + 1 if dx != 0 else 0
        sy, dyy = ys(dy, 2 * (CX - step), CY)
        return (CX // half, sy), (CX // half - dx, dyy)

    def within(cut, ref, *lead):
        def both(dx, dy):
            src, dst = cut(dx, dy)
            return ref.at[lead + src], ref.at[lead + dst]

        return both

    def exchange(directions, cut, send, recv):
        def copy(index, dx, dy):
            src, dst = cut(dx, dy)
            return pltpu.make_async_remote_copy(
                src_ref=src, dst_ref=dst, send_sem=send.at[index], recv_sem=recv.at[index],
                device_id=(slab + dx, cross + dy), device_id_type=MESH,
            )

        def start():
            for index, (dx, dy) in enumerate(directions):
                @pl.when(there(dx, dy))
                def _():
                    copy(index, dx, dy).start()

        def arrive():
            for index, (dx, dy) in enumerate(directions):
                @pl.when(there(-dx, -dy))
                def _():
                    copy(index, dx, dy).wait_recv()

        def leave():
            for index, (dx, dy) in enumerate(directions):
                @pl.when(there(dx, dy))
                def _():
                    copy(index, dx, dy).wait_send()

        return start, arrive, leave

    def fields_cut(dx, dy):
        return within(fine_cut, fields, slice(0, 2) if abs(dx) > 1 else slice(None))(dx, dy)

    f_x = exchange(NEAR, fields_cut, f_send, f_recv)
    m_x = exchange(WIDE, within(coarse_cut, packed_m), m_send, m_recv)
    r_x = [exchange(WIDE, within(coarse_cut, packed_r, at), r_send.at[at], r_recv.at[at]) for at in range(CYCLES)]
    p_x = [exchange(NEAR, within(fine_cut, press, at), p_send.at[at], p_recv.at[at]) for at in range(CYCLES)]

    def species_cut(dx, dy):
        if dx != 0:
            return species.at[:, cells_x - 1 if dx > 0 else 0], rim_x.at[0 if dx > 0 else 1]
        return species.at[:, :, cells_y - 1 if dy > 0 else 0], rim_y.at[0 if dy > 0 else 1]

    s_x = exchange(SIDE, species_cut, s_send, s_recv)

    def grids(rows):
        lane = lax.broadcasted_iota(jnp.int32, (rows, cells_z), 1)
        row = lax.broadcasted_iota(jnp.int32, (rows, cells_z), 0)
        return row, lane

    def next_z(v, k=1):
        return pltpu.roll(v, cells_z - k, 1)

    def prev_z(v, k=1):
        return pltpu.roll(v, k, 1)

    def next_y(v, k=1):
        return pltpu.roll(v, v.shape[0] - k, 0)

    def prev_y(v, k=1):
        return pltpu.roll(v, k, 0)

    row_w, lane_w = grids(wy)
    row_c, lane_c = grids(cy)
    row_o, lane_o = grids(cells_y)

    def pair_sum(v, row, lane):
        v = v + jnp.where(row % 2 == 0, next_y(v), prev_y(v))
        return v + jnp.where(lane % 2 == 0, next_z(v), prev_z(v))

    def pack(two):
        return jnp.where(lane_o % 2 == 0, two[0], two[1])

    def unpack(ref, dst):
        for block in range(2 * CX // half + 1):
            e = ref[block]
            dst[2 * block] = jnp.where(lane_c % 2 == 0, e, prev_z(e))
            dst[2 * block + 1] = jnp.where(lane_c % 2 == 0, next_z(e), e)

    inputs = [
        pltpu.make_async_copy(src, dst, in_sem.at[at])
        for at, (src, dst) in enumerate(((velocity_in, velocity), (density_in, density), (source_in, source)))
    ]
    for copy in inputs:
        copy.start()
    for ref in (fields, packed_m, packed_r, press, rim_x, rim_y):
        ref[...] = jnp.zeros(ref.shape, f32)
    barrier = pltpu.get_barrier_semaphore()
    count = jnp.int32(0)
    for dx, dy in WIDE:
        here = there(dx, dy)
        count = count + here.astype(jnp.int32)

        @pl.when(here)
        def _():
            pl.semaphore_signal(barrier, inc=1, device_id=(slab + dx, cross + dy), device_id_type=MESH)

    for copy in inputs:
        copy.wait()
    for x in range(cells_x):
        v2 = velocity[2, x]
        dz = jnp.where(lane_o == cells_z - 1, 0.0, next_z(v2)) - jnp.where(lane_o == 0, 0.0, prev_z(v2))
        fields[0, HX + x, own_y] = 1.0 / density[x]
        fields[1, HX + x, own_y] = velocity[0, x]
        fields[2, HX + x, own_y] = velocity[1, x]
        fields[3, HX + x, own_y] = 0.5 * dz - source[x]
    means = []
    for c in range(half):
        m = 1.0 / density[2 * c] + 1.0 / density[2 * c + 1]
        means.append(0.125 * pair_sum(m, row_o, lane_o))
    packed_m[CX // half, own_cy] = pack(means)
    pl.semaphore_wait(barrier, count)
    f_x[0]()
    m_x[0]()
    f_x[1]()

    def fine_setup(rows):
        for x in rows:
            m = fields[0, x]
            lo_x, hi_x = 0.5 * (m + fields[0, x - 1]), 0.5 * (m + fields[0, x + 1])
            lo_y, hi_y = 0.5 * (m + prev_y(m)), 0.5 * (m + next_y(m))
            lo_z = 0.5 * (m + jnp.where(lane_w == 0, 0.0, prev_z(m)))
            hi_z = 0.5 * (m + jnp.where(lane_w == cells_z - 1, 0.0, next_z(m)))
            diag = lo_x + hi_x + lo_y + hi_y + lo_z + hi_z
            inside = m > 0.0
            inv = jnp.where(inside, damping / jnp.where(inside, diag, 1.0), 0.0)
            xa[x], xb[x] = lo_x * inv, hi_x * inv
            ya[x], yb[x] = lo_y * inv, hi_y * inv
            za[x] = jnp.where(lane_w == 0, 0.0, lo_z * inv)
            zb[x] = jnp.where(lane_w == cells_z - 1, 0.0, hi_z * inv)
            if HX <= x < HX + cells_x:
                scale_back[x - HX] = (diag * (1.0 / damping))[HY : HY + cells_y]
            v1 = fields[2, x]
            t = 0.5 * ((fields[1, x + 1] - fields[1, x - 1]) + (next_y(v1) - prev_y(v1))) + fields[3, x]
            b = t * inv
            goal[x] = b
            pa[x] = -b

    early = range(HX - 2, HX + cells_x + 2)
    fine_setup(early)

    def sweep(src, dst, coefs, right, low, high, k):
        xl, xu, yl, yu, zl, zu = coefs
        for x in range(low, high):
            v = src[x]
            t = xl[x] * src[x - 1] + xu[x] * src[x + 1]
            t = t + (yl[x] * prev_y(v, k) + yu[x] * next_y(v, k))
            t = t + (zl[x] * prev_z(v, k) + zu[x] * next_z(v, k))
            dst[x] = (1.0 - damping) * v + (t - right[x])

    fine = (xa, xb, ya, yb, za, zb)
    coarse = (cxa, cxb, cya, cyb, cza, czb)

    def coarse_setup(rows):
        for x in rows:
            m = coarse_m[x]
            lo_x, hi_x = 0.5 * (m + coarse_m[x - 1]), 0.5 * (m + coarse_m[x + 1])
            lo_y, hi_y = 0.5 * (m + prev_y(m, 2)), 0.5 * (m + next_y(m, 2))
            lo_z = 0.5 * (m + jnp.where(lane_c < 2, 0.0, prev_z(m, 2)))
            hi_z = 0.5 * (m + jnp.where(lane_c >= cells_z - 2, 0.0, next_z(m, 2)))
            diag = lo_x + hi_x + lo_y + hi_y + lo_z + hi_z
            inside = m > 0.0
            inv = jnp.where(inside, damping / jnp.where(inside, diag, 1.0), 0.0)
            cxa[x], cxb[x] = lo_x * inv, hi_x * inv
            cya[x], cyb[x] = lo_y * inv, hi_y * inv
            cza[x] = jnp.where(lane_c < 2, 0.0, lo_z * inv)
            czb[x] = jnp.where(lane_c >= cells_z - 2, 0.0, hi_z * inv)
            if CX <= x < CX + half:
                cinv[x - CX] = inv[CY : CY + cells_y]

    def correct(at, pre, free, reach):
        for x in range(HX, HX + cells_x):
            press[at, x, own_y] = pre[x, own_y]
        own_rows = range(CX, CX + half)
        if at == 0:
            m_x[1]()
            unpack(packed_m, coarse_m)
            coarse_setup(own_rows)
        sums = []
        for c in range(half):
            r = None
            for x in (HX + 2 * c, HX + 2 * c + 1):
                v = pre[x]
                t = xa[x] * pre[x - 1] + xb[x] * pre[x + 1]
                t = t + (ya[x] * prev_y(v) + yb[x] * next_y(v))
                t = t + (za[x] * prev_z(v) + zb[x] * next_z(v))
                d = (damping * v - (t - goal[x]))[HY : HY + cells_y] * scale_back[x - HX]
                r = d if r is None else r + d
            sums.append(0.5 * pair_sum(r, row_o, lane_o) * cinv[c])
        packed_r[at, CX // half, own_cy] = pack(sums)
        r_x[at][0]()
        p_x[at][0]()
        if at == 0:
            s_x[0]()
            coarse_setup([x for x in range(1, cw - 1) if x not in own_rows])
            fine_setup([x for x in range(1, wx - 1) if x not in early])
        r_x[at][1]()
        unpack(packed_r.at[at], right)
        for x in range(cw):
            ca[x] = -right[x]
        src, dst = ca, cb
        for step in range(1, COARSE):
            sweep(src, dst, coarse, right, step, cw - step, 2)
            src, dst = dst, src
        p_x[at][1]()
        low, high = HX - reach - 2, HX + cells_x + reach + 2
        for x in range(low, high):
            pre[x] = press[at, x] + src[CX + (x - HX) // 2, pl.ds(CY - HY, wy)]
        sweep(pre, free, fine, goal, low + 1, high - 1, 1)
        sweep(free, pre, fine, goal, low + 2, high - 2, 1)

    sweep(pa, pb, fine, goal, HX - 1, HX + cells_x + 1, 1)
    correct(0, pb, pa, 3)
    sweep(pb, pa, fine, goal, HX - 2, HX + cells_x + 2, 1)
    sweep(pa, pb, fine, goal, HX - 1, HX + cells_x + 1, 1)
    correct(1, pb, pa, 2)
    last = pb

    for x in range(HX - 1, HX + cells_x + 1):
        grad = 0.5 * (last[x + 1, own_y] - last[x - 1, own_y])
        out_x[x - HX + 1] = fields[1, x, own_y] - fields[0, x, own_y] * grad
    for x in range(cells_x):
        w = x + HX
        v = last[w]
        out_y[x] = fields[2, w] - fields[0, w] * (0.5 * (next_y(v) - prev_y(v)))
        own = v[HY : HY + cells_y]
        dz = jnp.where(lane_o == cells_z - 1, 0.0, next_z(own)) - jnp.where(lane_o == 0, 0.0, prev_z(own))
        out_z[x] = velocity[2, x] - fields[0, w, own_y] * (0.5 * dz)
        out_p[x] = own
    s_x[1]()
    for x in (f_x, m_x, s_x, *r_x, *p_x):
        x[2]()


def transport(in_x, in_y, in_z, in_p, rim_x, rim_y, species, vel_out, pres_out, spec_out):
    cells_x, cells_y, cells_z = in_p.shape
    lane_o = lax.broadcasted_iota(jnp.int32, (cells_y, cells_z), 1)
    row_o = lax.broadcasted_iota(jnp.int32, (cells_y, cells_z), 0)

    def next_z(v):
        return pltpu.roll(v, cells_z - 1, 1)

    def prev_z(v):
        return pltpu.roll(v, 1, 1)

    def next_y(v):
        return pltpu.roll(v, v.shape[0] - 1, 0)

    def prev_y(v):
        return pltpu.roll(v, 1, 0)

    mid = slice(HY, HY + cells_y)
    pres_out[...] = in_p[...]
    move_x = [in_x[x] for x in range(cells_x + 2)]
    for x in range(cells_x):
        move_y, move_z = in_y[x], in_z[x]
        vel_out[0, x] = move_x[x + 1]
        vel_out[1, x] = move_y[mid]
        vel_out[2, x] = move_z
        lo_x, hi_x = 0.5 * (move_x[x] + move_x[x + 1]), 0.5 * (move_x[x + 1] + move_x[x + 2])
        lo_y, hi_y = (0.5 * (move_y + prev_y(move_y)))[mid], (0.5 * (move_y + next_y(move_y)))[mid]
        lo_z = 0.5 * (move_z + jnp.where(lane_o == 0, 0.0, prev_z(move_z)))
        hi_z = 0.5 * (move_z + jnp.where(lane_o == cells_z - 1, 0.0, next_z(move_z)))

        def into(flow):
            return time_step * jnp.maximum(flow, 0.0)

        def back(flow):
            return -time_step * jnp.minimum(flow, 0.0)

        keep = 1.0 - (into(hi_x) + into(hi_y) + into(hi_z)) - (back(lo_x) + back(lo_y) + back(lo_z))
        from_xl, from_xu = into(lo_x), back(hi_x)
        from_yl, from_yu = into(lo_y), back(hi_y)
        from_zl = jnp.where(lane_o == 0, 0.0, into(lo_z))
        from_zu = jnp.where(lane_o == cells_z - 1, 0.0, back(hi_z))
        for s in range(species.shape[0]):
            q = species[s, x]
            xl = rim_x[0, s] if x == 0 else species[s, x - 1]
            xu = rim_x[1, s] if x == cells_x - 1 else species[s, x + 1]
            yl = jnp.where(row_o == 0, rim_y[0, s, pl.ds(x, 1)], prev_y(q))
            yu = jnp.where(row_o == cells_y - 1, rim_y[1, s, pl.ds(x, 1)], next_y(q))
            total = keep * q + (from_xl * xl + from_xu * xu) + (from_yl * yl + from_yu * yu)
            spec_out[s, x] = total + (from_zl * prev_z(q) + from_zu * next_z(q))


def local(slabs, crosses, velocity, density, source, species):
    cells_x, cells_y, cells_z = density.shape
    assert cells_x == 4 and CX % (cells_x // 2) == 0 and cells_y % 8 == 0 and cells_y >= CY
    wx, wy = cells_x + 2 * HX, cells_y + 2 * HY
    half = cells_x // 2
    kinds = species.shape[0]
    f32 = jnp.float32

    def vmem(*shape):
        return pltpu.VMEM(shape, f32)

    fine, coarse = (wx, wy, cells_z), (half + 2 * CX, cells_y + 2 * CY, cells_z)
    packed = (2 * CX // half + 1,) + coarse[1:]
    near, wide, side = len(NEAR), len(WIDE), len(SIDE)
    dma = pltpu.SemaphoreType.DMA
    spec = pl.BlockSpec(memory_space=pltpu.VMEM)
    anywhere = pl.BlockSpec(memory_space=pl.ANY)
    moved = [
        (cells_x + 2, cells_y, cells_z), (cells_x, wy, cells_z), density.shape, density.shape,
        (2, kinds, cells_y, cells_z), (2, kinds, cells_x, cells_z),
    ]
    between = pl.pallas_call(
        functools.partial(kernel, slabs, crosses),
        out_shape=tuple(jax.ShapeDtypeStruct(shape, f32) for shape in moved),
        in_specs=[anywhere] * 4,
        out_specs=(spec,) * 6,
        scratch_shapes=[vmem(*velocity.shape), vmem(*density.shape), vmem(*density.shape)]
        + [vmem(4, *fine), vmem(*packed), vmem(CYCLES, *packed), vmem(CYCLES, *fine)]
        + [vmem(*coarse)] * 2
        + [vmem(*fine)] * 7 + [vmem(*density.shape)] + [vmem(*fine)] * 2
        + [vmem(*coarse)] * 6 + [vmem(half, cells_y, cells_z)] + [vmem(*coarse)] * 2
        + [dma((3,))] + [dma((near,))] * 2 + [dma((wide,))] * 2
        + [dma((CYCLES, wide))] * 2 + [dma((CYCLES, near))] * 2 + [dma((side,))] * 2,
        compiler_params=pltpu.CompilerParams(collective_id=0, has_side_effects=True),
        name="projection",
    )(velocity, density, source, species)
    return pl.pallas_call(
        transport,
        out_shape=tuple(jax.ShapeDtypeStruct(a.shape, f32) for a in (velocity, density, species)),
        in_specs=[spec] * 7,
        out_specs=(spec,) * 3,
        name="transport",
    )(*between, species)


def solution(mesh):
    plane, stack = P("slab", "cross", None), P(None, "slab", "cross", None)
    return jax.shard_map(
        functools.partial(local, mesh.shape["slab"], mesh.shape["cross"]),
        mesh=mesh,
        in_specs=(stack, plane, plane, stack),
        out_specs=(stack, plane, stack),
        check_vma=False,
    )
```
